32 devices in a mesh: gx: 8 (over y, x, core), gy: 4 (over z).
Axes of the slice: x: 2, y: 2, z: 4, core: 2. Of those that a mesh axis runs over, the one named last changes fastest.
Arguments:
- sat_new: float32 [64, 512, 512], P(None, 'gx', 'gy'), may hold values from 0.02 to 1
- sat_old: float32 [64, 512, 512], P(None, 'gx', 'gy'), may hold values from 0.1 to 0.95
- porosity: float32 [64, 512, 512], P(None, 'gx', 'gy'), may hold values from 0.1 to 0.5
- spec_storage: float32 [64, 512, 512], P(None, 'gx', 'gy'), may hold values from 0.01 to 0.2
- pressure: float32 [64, 512, 512], P(None, 'gx', 'gy'), may hold values from -6 to 6
- conduct: float32 [64, 512, 512], P(None, 'gx', 'gy'), may hold values from 0.1 to 1
- et_rate: float32 [64, 512, 512], P(None, 'gx', 'gy'), may hold values from 0 to 1
- thickness: float32 [64], replicated, may hold values from 0.005 to 0.05
- labels: int32 [512, 512], P('gx', 'gy'), may hold values from 0 to 511, as said below
- outlet: int32 [512, 512], P('gx', 'gy'), may hold values 0 or 1
Outputs:
- basin_totals: float32 [4, 64, 512], replicated
- column_balance: float32 [4, 512, 512], P(None, 'gx', 'gy')
- peak_change: float32 [], replicated
The draws below stay inside these ranges and needn't reach their ends.
Inputs may be any that keep to these rules, and one draw needn't show every extreme that they name: `labels`: subbasins are contiguous patches of columns with ragged edges.
All inputs are finite; a program needn't handle non-finite values. No bound on the sum of `outlet` on one device may be relied on, other than what follows from the above.
Results may differ from the reference program's by a relative error of at most 0.00016.
Values sent between devices are 32-bit elements; how exact they have to be, the bound alone decides.
A program may use at most 128 MiB of HBM per device.

```python
import math
import jax
import jax.numpy as jnp

NZ = 64
SUB = 512
CX = 64
CY = 128
NX = 512
NY = 512


def saturation_pair(key):
    first, second, third = jax.random.split(jax.random.fold_in(key, 7301), 3)
    older = jax.random.uniform(first, (NZ, NX, NY), jnp.float32, 0.2, 0.9)
    noise = jax.random.normal(second, (NZ, NX, NY), jnp.float32)
    blocks_x = NX // CX
    blocks_y = NY // CY
    amp_log = jax.random.uniform(third, (blocks_x, blocks_y), jnp.float32, jnp.log(0.01), jnp.log(0.3))
    amp = jnp.exp(amp_log)
    amp_full = jnp.repeat(jnp.repeat(amp, CX, axis=0), CY, axis=1)
    newer = jnp.clip(older + noise * amp_full[None], 0.02, 1.0)
    return (older, newer)


def draw_sat_new(key, part):
    older, newer = saturation_pair(key)
    return newer


def draw_sat_old(key, part):
    older, newer = saturation_pair(key)
    return older


def draw_labels(key, part):
    first, second, third = jax.random.split(jax.random.fold_in(key, 911), 3)
    rows_x = jnp.arange(NX, dtype=jnp.int32)[:, None]
    rows_y = jnp.arange(NY, dtype=jnp.int32)[None, :]
    jitter_x = jax.random.randint(first, (NX, NY), -4, 5, dtype=jnp.int32)
    jitter_y = jax.random.randint(second, (NX, NY), -4, 5, dtype=jnp.int32)
    moved_x = jnp.clip(rows_x + jitter_x, 0, NX - 1)
    moved_y = jnp.clip(rows_y + jitter_y, 0, NY - 1)
    across = SUB // 32
    region = moved_x * 32 // NX * across + moved_y * across // NY
    order = jax.random.permutation(third, SUB).astype(jnp.int32)
    return order[region].astype(jnp.int32)


def with_ends(drawn, own_key, smallest, top_value):
    longest = drawn.shape.index(max(drawn.shape))
    spots = []
    for shift in (0, 1):
        where = [jax.random.randint(jax.random.fold_in(own_key, axis), (), 0, length) for axis, length in enumerate(drawn.shape)]
        where[longest] = (where[longest] + shift) % drawn.shape[longest]
        spots.append(tuple(where))
    return drawn.at[spots[0]].set(smallest).at[spots[1]].set(top_value)


def block_scale(stream_key, shape, shards, least, top_value):
    def one(position, shards_of):
        steps = jax.random.uniform(jax.random.fold_in(jax.random.fold_in(stream_key, 6), position), (shards_of,), jnp.float32, least / len(shards), top_value / len(shards))
        return jnp.repeat(jnp.exp(steps), shape[position] // shards_of).reshape((-1,) + (1,) * (len(shape) - position - 1))

    level = one(*shards[0])
    for cut in shards[1:]:
        level = level * one(*cut)
    return level


def scatter_about(key, extent, deviation, most, cuts=(), kind=jnp.bfloat16):
    gain = block_scale(key, extent, cuts, -0.22, 0.18) if cuts else 1.0
    result = jax.random.normal(key, extent, jnp.float32) * deviation * gain
    return jnp.minimum(jnp.maximum(result, -most), most).astype(kind)


def setup_inputs(seed: int = 0) -> dict:
    streams_of = jax.random.split(jax.random.key(seed), 11)
    sat_new = draw_sat_new(jax.random.fold_in(streams_of[10], 71), 0)
    sat_old = draw_sat_old(jax.random.fold_in(streams_of[10], 71), 0)
    porosity = jnp.clip(0.1 + 0.4 * jax.random.uniform(streams_of[2], (NZ, NX, NY), jnp.float32) ** block_scale(streams_of[2], (NZ, NX, NY), ((1, 8), (2, 4)), -0.2, 0.2), 0.1, 0.5)
    spec_storage = jnp.clip(jnp.exp(math.log(0.2) - 2.9957323 * jax.random.uniform(streams_of[3], (NZ, NX, NY), jnp.float32) ** block_scale(streams_of[3], (NZ, NX, NY), ((1, 8), (2, 4)), -0.2, 0.2)), 0.01, 0.2)
    pressure = scatter_about(streams_of[4], (NZ, NX, NY), 1.0, 6.0, ((1, 8), (2, 4)), jnp.float32)
    conduct = jnp.clip(jnp.exp(math.log(1.0) - 2.3025851 * jax.random.uniform(streams_of[5], (NZ, NX, NY), jnp.float32) ** block_scale(streams_of[5], (NZ, NX, NY), ((1, 8), (2, 4)), -0.2, 0.2)), 0.1, 1.0)
    et_rate = jnp.clip(1.0 * jax.random.uniform(streams_of[6], (NZ, NX, NY), jnp.float32) ** block_scale(streams_of[6], (NZ, NX, NY), ((1, 8), (2, 4)), -0.2, 0.2), 0.0, 1.0)
    thickness = jnp.clip(jnp.exp(jax.random.uniform(streams_of[7], (NZ,), jnp.float32, math.log(0.005), math.log(0.05))), 0.005, 0.05)
    labels = draw_labels(jax.random.fold_in(streams_of[10], 71), 0)
    outlet = with_ends((jax.random.randint(streams_of[9], (NX, NY), 0, 8) < 1).astype(jnp.int32), jax.random.fold_in(streams_of[9], 1), 0, 1)
    return dict(sat_new=sat_new, sat_old=sat_old, porosity=porosity, spec_storage=spec_storage, pressure=pressure, conduct=conduct, et_rate=et_rate, thickness=thickness, labels=labels, outlet=outlet)


def lateral_flux(pressure, conduct, depth):
    padded_p = jnp.pad(pressure, ((0, 0), (1, 1), (1, 1)))
    padded_k = jnp.pad(conduct, ((0, 0), (1, 1), (1, 1)))
    cx = pressure.shape[1]
    cy = pressure.shape[2]
    total = jnp.zeros(pressure.shape, jnp.float32)
    for shift_i, shift_j in ((0, 1), (2, 1), (1, 0), (1, 2)):
        near_p = padded_p[:, shift_i:shift_i + cx, shift_j:shift_j + cy]
        near_k = padded_k[:, shift_i:shift_i + cx, shift_j:shift_j + cy]
        face = 2.0 * conduct * near_k / (conduct + near_k)
        total = total + face * (pressure - near_p)
    return depth * total


def reference(sat_new, sat_old, porosity, spec_storage, pressure, conduct, et_rate, thickness, labels, outlet):
    depth = thickness[:, None, None]
    flux = lateral_flux(pressure, conduct, depth)
    water = depth * sat_new * (porosity + spec_storage * pressure)
    change = depth * porosity * (sat_new - sat_old)
    uptake = depth * et_rate
    fields = jnp.stack([water, change, uptake, flux])
    column_balance = jnp.sum(fields, axis=1)
    masked = jnp.concatenate([fields[:3], fields[3:] * outlet.astype(jnp.float32)[None, None]], axis=0)
    rows = masked.reshape(4 * NZ, NX * NY)
    flat_labels = labels.reshape(-1).astype(jnp.int32)
    summed = jax.ops.segment_sum(rows.T, flat_labels, num_segments=SUB)
    basin_scale = NZ * SUB / (NX * NY)
    basin_totals = (summed.T.reshape(4, NZ, SUB) * basin_scale).astype(jnp.float32)
    peak_change = jnp.max(jnp.abs(sat_new - sat_old))
    return basin_totals, column_balance, peak_change
```

```python
import functools

import jax
import jax.numpy as jnp
from jax import lax
from jax.experimental import pallas as pl
from jax.experimental.pallas import tpu as pltpu
from jax.sharding import PartitionSpec as P

SUB = 512
LANES = 128
STEP = 8
GROUP = 4
ZBLOCK = 32
MESH = pl.DeviceIdType.MESH
VMEM_LIMIT = 60 * 1024 * 1024


def flow(p, k, pn, kn):
    return 2.0 * k * kn / (k + kn) * (p - pn)


def split(value):
    high = value.astype(jnp.bfloat16)
    return high, (value - high.astype(jnp.float32)).astype(jnp.bfloat16)


def spread(thick_row, layers):
    rows = lax.broadcasted_iota(jnp.int32, (layers, layers), 0)
    cols = lax.broadcasted_iota(jnp.int32, (layers, layers), 1)
    grid = jnp.broadcast_to(thick_row, (layers, layers))
    column = jnp.sum(jnp.where(rows == cols, grid, 0.0), axis=1, keepdims=True)
    return jnp.broadcast_to(column, (layers, LANES))


def onehot_of(row):
    ids = lax.broadcasted_iota(jnp.int32, (SUB, LANES), 0)
    return jnp.where(ids == row, 1.0, 0.0).astype(jnp.bfloat16)


def nt_dot(a, b):
    return lax.dot_general(
        a, b, (((1,), (1,)), ((), ())), preferred_element_type=jnp.float32
    )


def local_kernel(
    pressure, conduct, sat_new, sat_old, porosity, storage, et_rate, thick, labels, outlet,
    partial, balance, edges, peak,
    p_buf, k_buf, n_buf, o_buf, r_buf, s_buf, e_buf, depth, carry, sums, lhs, hot, total, sems,
):
    layers, cx, cy = pressure.shape
    chunks = cx // STEP
    first = ((pressure, p_buf), (conduct, k_buf))
    rest = ((sat_new, n_buf), (sat_old, o_buf), (porosity, r_buf), (storage, s_buf), (et_rate, e_buf))
    pairs = first + rest

    def fetch(chunk, which):
        for a in which:
            source, target = pairs[a]
            for i in range(STEP):
                x = chunk * STEP + i
                pltpu.make_async_copy(source.at[:, x, :], target.at[x], sems.at[a, chunk]).start()

    def wait(chunk, which):
        for a in which:
            target = pairs[a][1].at[pl.ds(chunk * STEP, STEP)]
            pltpu.make_async_copy(target, target, sems.at[a, chunk]).wait()

    fetch(0, (0, 1))
    for chunk in range(chunks):
        if chunk + 1 < chunks:
            fetch(chunk + 1, (0, 1))
        fetch(chunk, range(2, 7))

    p_buf[cx] = jnp.zeros((layers, cy), jnp.float32)
    k_buf[cx] = jnp.zeros((layers, cy), jnp.float32)
    depth[...] = spread(thick[...], layers)
    carry[...] = jnp.zeros_like(carry)
    total[...] = jnp.zeros_like(total)
    peak[...] = jnp.zeros_like(peak)
    sums[...] = jnp.zeros_like(sums)
    edges[:, 2] = jnp.zeros((2, layers, cy), jnp.float32)
    lane = lax.broadcasted_iota(jnp.int32, (ZBLOCK, cy), 1)
    quarter = 4 * layers
    wait(0, (0, 1))

    def fold(value):
        return jnp.sum(value.reshape(ZBLOCK // 8, 8, cy), axis=0)

    def body(chunk, _):
        @pl.when(chunk + 1 < chunks)
        def _():
            wait(chunk + 1, (0, 1))

        wait(chunk, range(2, 7))
        for sub in range(STEP // GROUP):
            for zi in range(layers // ZBLOCK):
                zs = pl.ds(zi * ZBLOCK, ZBLOCK)
                before = carry[zs]
                d = depth[zs]
                biggest = peak[...]
                for i in range(GROUP):
                    x = chunk * STEP + sub * GROUP + i
                    p = p_buf[x, zs]
                    k = k_buf[x, zs]
                    ahead = flow(p, k, p_buf[x + 1, zs], k_buf[x + 1, zs])
                    side = flow(p, k, pltpu.roll(p, cy - 1, 1), pltpu.roll(k, cy - 1, 1))
                    side = jnp.where(lane < cy - 1, side, 0.0)
                    flux = d * (ahead - before + side - pltpu.roll(side, 1, 1))
                    before = ahead
                    mine = (lane >> 1) == x
                    edges[0, 2, zs] = jnp.where(mine, pltpu.roll(p, 2 * x + 1, 1), edges[0, 2, zs])
                    edges[1, 2, zs] = jnp.where(mine, pltpu.roll(k, 2 * x + 1, 1), edges[1, 2, zs])
                    new = n_buf[x, zs]
                    delta = new - o_buf[x, zs]
                    por = r_buf[x, zs]
                    water = d * new * (por + s_buf[x, zs] * p)
                    change = d * por * delta
                    uptake = d * e_buf[x, zs]
                    biggest = jnp.maximum(
                        biggest, jnp.max(jnp.abs(delta).reshape(ZBLOCK // 8, 8, cy), axis=0)
                    )
                    gate = outlet[pl.ds(x, 1), :].astype(jnp.float32)
                    cols = pl.ds(i * cy, cy)
                    for q, (field, kept) in enumerate(
                        ((water, water), (change, change), (uptake, uptake), (flux, flux * gate))
                    ):
                        sums[q, x] += fold(field)
                        high, low = split(kept)
                        row = q * layers + zi * ZBLOCK
                        lhs[sub, pl.ds(row, ZBLOCK), cols] = high
                        lhs[sub, pl.ds(quarter + row, ZBLOCK), cols] = low
                carry[zs] = before
                peak[...] = biggest
            for i in range(GROUP):
                x = chunk * STEP + sub * GROUP + i
                hot[sub, :, pl.ds(i * cy, cy)] = onehot_of(labels[pl.ds(x, 1), :])
            out = nt_dot(lhs[sub], hot[sub])
            total[...] += out[:quarter] + out[quarter:]
        return 0

    lax.fori_loop(0, chunks, body, 0)
    for c in range(SUB // LANES):
        partial[pl.ds(c * quarter, quarter)] = total[:, pl.ds(c * LANES, LANES)]
    for q in range(4):
        balance[q] = jnp.sum(sums[q], axis=1)
    for a, buf in enumerate((p_buf, k_buf)):
        edges[a, 0] = buf[0]
        edges[a, 1] = buf[cx - 1]


def stages_of(n1, n2):
    found = []
    if n1 % 2 == 0 and n1 > 2:
        found += [("gx", 1, 2), ("gx", 2, n1 // 2)]
    else:
        found += [("gx", 1, n1)]
    return found + [("gy", 1, n2)]


def shared_kernel(
    n1, n2, scale,
    partial, balance_in, edges, peak_in, thick, labels, outlet,
    totals, balance, peak,
    halo, work, *rest,
):
    stages = stages_of(n1, n2)
    count = len(stages)
    slots = rest[:count]
    blocks = rest[count : 2 * count]
    tiles = rest[2 * count : 3 * count]
    tops, full, halo_send, halo_recv, send, recv, tile_send, tile_recv, back_send, back_recv = rest[3 * count :]
    gx = lax.axis_index("gx")
    gy = lax.axis_index("gy")
    layers = edges.shape[2]
    cx = labels.shape[0]
    cy = labels.shape[1]
    quarter = 4 * layers

    barrier = pltpu.get_barrier_semaphore()
    for axis, me, n in (("gx", gx, n1), ("gy", gy, n2)):
        for j in range(1, n):
            pl.semaphore_signal(barrier, inc=1, device_id={axis: lax.rem(me + j, n)}, device_id_type=MESH)
    pl.semaphore_wait(barrier, n1 + n2 - 2)

    copies = []
    for slot, (axis, me, n, hop, which) in enumerate(
        (("gx", gx, n1, 1, 1), ("gx", gx, n1, n1 - 1, 0), ("gy", gy, n2, 1, 2), ("gy", gy, n2, n2 - 1, 2))
    ):
        copy = pltpu.make_async_remote_copy(
            src_ref=edges.at[:, which],
            dst_ref=halo.at[slot],
            send_sem=halo_send.at[slot],
            recv_sem=halo_recv.at[slot],
            device_id={axis: lax.rem(me + hop, n)},
            device_id_type=MESH,
        )
        copy.start()
        copies.append(copy)

    depth = spread(thick[...], layers)
    lane = lax.broadcasted_iota(jnp.int32, (layers, cy), 1)
    place_x = lax.broadcasted_iota(jnp.int32, (cx, cy), 0)
    place_c = lax.broadcasted_iota(jnp.int32, (cx, cy), 1)

    def packed(grid):
        top = jnp.broadcast_to(grid[:, cy - 1 :], (cx, cy))
        low = jnp.broadcast_to(grid[:, :1], (cx, cy))
        spot = jnp.where(place_c == 2 * place_x, top, 0) + jnp.where(place_c == 2 * place_x + 1, low, 0)
        return jnp.sum(spot, axis=0, keepdims=True)

    work[...] = partial[...]
    gates = outlet[...].astype(jnp.float32)
    names = labels[...].astype(jnp.float32)
    side_names = packed(names).astype(jnp.int32)
    side_gates = packed(gates)
    hot = jnp.concatenate(
        [onehot_of(labels[pl.ds(0, 1), :]), onehot_of(labels[pl.ds(cx - 1, 1), :]), onehot_of(side_names)], axis=1
    )

    for copy in copies:
        copy.wait()
    inside = (gx > 0, gx < n1 - 1, gy > 0, gy < n2 - 1)
    open_ = [jnp.where(flag, 1.0, 0.0) for flag in inside]
    near_p = [halo[s, 0] for s in range(4)]
    near_k = [halo[s, 1] * open_[s] for s in range(4)]
    low = depth * flow(edges[0, 0], edges[1, 0], near_p[0], near_k[0])
    high = depth * flow(edges[0, 1], edges[1, 1], near_p[1], near_k[1])
    even = (lane & 1) == 0
    side_p = jnp.where(even, pltpu.roll(near_p[3], cy - 1, 1), pltpu.roll(near_p[2], 1, 1))
    side_k = jnp.where(even, pltpu.roll(near_k[3], cy - 1, 1), pltpu.roll(near_k[2], 1, 1))
    own_k = edges[1, 2]
    own_k = jnp.where(lane < 2 * cx, own_k, 1.0)
    side = depth * flow(edges[0, 2], own_k, side_p, side_k)
    side = jnp.where(lane < 2 * cx, side, 0.0)
    extra = jnp.concatenate(
        [low * gates[:1], high * gates[cx - 1 :], side * side_gates], axis=1
    )
    up, down = split(extra)
    out = nt_dot(jnp.concatenate([up, down], axis=0), hot)
    out = out[:layers] + out[layers:]
    for c in range(SUB // LANES):
        work[pl.ds(c * quarter + 3 * layers, layers)] += out[:, c * LANES : (c + 1) * LANES]

    current = work
    rows = SUB // LANES * quarter
    base = 0
    pending = []
    tops[0] = peak_in[...]
    for s, (axis, stride, size) in enumerate(stages):
        me = gx if axis == "gx" else gy
        spot = lax.rem(me // stride, size)
        part = rows // size
        step_copies = []
        for j in range(1, size):
            there = lax.rem(spot + j, size)
            target = me + (there - spot) * stride
            begin = pl.multiple_of(there * part, 8)
            copy = pltpu.make_async_remote_copy(
                src_ref=current.at[pl.ds(begin, part)],
                dst_ref=slots[s].at[j - 1],
                send_sem=send.at[s, j - 1],
                recv_sem=recv.at[s, j - 1],
                device_id={axis: target},
                device_id_type=MESH,
            )
            copy.start()
            step_copies.append(copy)
            copy = pltpu.make_async_remote_copy(
                src_ref=tops.at[s],
                dst_ref=tiles[s].at[j - 1],
                send_sem=tile_send.at[s, j - 1],
                recv_sem=tile_recv.at[s, j - 1],
                device_id={axis: target},
                device_id_type=MESH,
            )
            copy.start()
            step_copies.append(copy)
        for copy in step_copies:
            copy.wait_recv()
        pending += step_copies
        mine = pl.multiple_of(spot * part, 8)
        value = current[pl.ds(mine, part)]
        top = tops[s]
        for j in range(size - 1):
            value = value + slots[s][j]
            top = jnp.maximum(top, tiles[s][j])
        tops[s + 1] = top
        base = base + spot * part
        rows = part
        if s + 1 < count:
            blocks[s][...] = value
            current = blocks[s]
        else:
            full[pl.ds(pl.multiple_of(base, 8), part)] = value * scale

    for s in range(count - 1, -1, -1):
        axis, stride, size = stages[s]
        me = gx if axis == "gx" else gy
        spot = lax.rem(me // stride, size)
        held = full.at[pl.ds(pl.multiple_of(base, 8), rows)]
        step_copies = []
        for j in range(1, size):
            there = lax.rem(spot + j, size)
            copy = pltpu.make_async_remote_copy(
                src_ref=held,
                dst_ref=held,
                send_sem=back_send.at[s, j - 1],
                recv_sem=back_recv.at[s, j - 1],
                device_id={axis: me + (there - spot) * stride},
                device_id_type=MESH,
            )
            copy.start()
            step_copies.append(copy)
        if s == count - 1:
            sum_low = jnp.sum(low, axis=0, keepdims=True)
            sum_high = jnp.sum(high, axis=0, keepdims=True)
            sum_side = jnp.broadcast_to(jnp.sum(side, axis=0, keepdims=True), (cx, cy))
            column_top = jnp.sum(jnp.where(place_c == 2 * place_x, sum_side, 0.0), axis=1, keepdims=True)
            column_low = jnp.sum(jnp.where(place_c == 2 * place_x + 1, sum_side, 0.0), axis=1, keepdims=True)
            more = jnp.where(place_c == cy - 1, column_top, 0.0) + jnp.where(place_c == 0, column_low, 0.0)
            more = more + jnp.where(place_x == 0, sum_low, 0.0) + jnp.where(place_x == cx - 1, sum_high, 0.0)
            balance[pl.ds(0, 3)] = balance_in[pl.ds(0, 3)]
            balance[3] = balance_in[3] + more
            best = jnp.max(jnp.max(tops[count], axis=0, keepdims=True), axis=1, keepdims=True)
            peak[...] = best
        for copy in step_copies:
            copy.wait_recv()
        pending += step_copies
        base = base - spot * rows
        rows = rows * size
    for c in range(SUB // LANES):
        for q in range(4):
            totals[q, :, pl.ds(c * LANES, LANES)] = full[pl.ds(c * quarter + q * layers, layers)]
    for copy in pending:
        copy.wait_send()


def on_device(
    n1, n2,
    sat_new, sat_old, porosity, spec_storage, pressure, conduct, et_rate, thickness, labels, outlet
):
    layers, cx, cy = sat_new.shape
    quarter = 4 * layers
    f32 = jnp.float32
    vmem = pl.BlockSpec(memory_space=pltpu.VMEM)
    hbm = pl.BlockSpec(memory_space=pl.ANY)
    rows = SUB // LANES * quarter
    thick = thickness.reshape(1, layers)
    slab = pltpu.VMEM((cx, layers, cy), f32)
    slab1 = pltpu.VMEM((cx + 1, layers, cy), f32)
    partial, balance, edges, peak = pl.pallas_call(
        local_kernel,
        out_shape=(
            jax.ShapeDtypeStruct((rows, LANES), f32),
            jax.ShapeDtypeStruct((4, cx, cy), f32),
            jax.ShapeDtypeStruct((2, 3, layers, cy), f32),
            jax.ShapeDtypeStruct((8, cy), f32),
        ),
        in_specs=[hbm] * 7 + [vmem] * 3,
        out_specs=(vmem,) * 4,
        scratch_shapes=[slab1, slab1] + [slab] * 5 + [
            pltpu.VMEM((layers, cy), f32),
            pltpu.VMEM((layers, cy), f32),
            pltpu.VMEM((4, cx, 8, cy), f32),
            pltpu.VMEM((STEP // GROUP, 2 * quarter, GROUP * cy), jnp.bfloat16),
            pltpu.VMEM((STEP // GROUP, SUB, GROUP * cy), jnp.bfloat16),
            pltpu.VMEM((quarter, SUB), f32),
            pltpu.SemaphoreType.DMA((7, cx // STEP)),
        ],
        compiler_params=pltpu.CompilerParams(vmem_limit_bytes=VMEM_LIMIT),
        name="local",
    )(pressure, conduct, sat_new, sat_old, porosity, spec_storage, et_rate, thick, labels, outlet)

    stages = stages_of(n1, n2)
    count = len(stages)
    widest = max(size for _, _, size in stages) - 1
    left = rows
    slots, blocks, tiles = [], [], []
    for _, _, size in stages:
        left //= size
        slots.append(pltpu.VMEM((size - 1, left, LANES), f32))
        blocks.append(pltpu.VMEM((left, LANES), f32))
        tiles.append(pltpu.VMEM((size - 1, 8, LANES), f32))
    dma = pltpu.SemaphoreType.DMA
    scale = layers * SUB / (cx * n1 * cy * n2)
    totals, balance, peak = pl.pallas_call(
        functools.partial(shared_kernel, n1, n2, scale),
        out_shape=(
            jax.ShapeDtypeStruct((4, layers, SUB), f32),
            jax.ShapeDtypeStruct((4, cx, cy), f32),
            jax.ShapeDtypeStruct((1, 1), f32),
        ),
        in_specs=[vmem] * 7,
        out_specs=(vmem,) * 3,
        scratch_shapes=[
            pltpu.VMEM((4, 2, layers, cy), f32),
            pltpu.VMEM((rows, LANES), f32),
            *slots, *blocks, *tiles,
            pltpu.VMEM((count + 1, 8, LANES), f32),
            pltpu.VMEM((rows, LANES), f32),
            dma((4,)), dma((4,)),
        ] + [dma((count, widest))] * 6,
        compiler_params=pltpu.CompilerParams(
            collective_id=0, has_side_effects=True, vmem_limit_bytes=32 * 1024 * 1024
        ),
        name="shared",
    )(partial, balance, edges, peak, thick, labels, outlet)
    return totals, balance, peak[0, 0]


def solution(mesh):
    columns = P(None, "gx", "gy")
    in_specs = (columns,) * 7 + (P(), P("gx", "gy"), P("gx", "gy"))
    out_specs = (P(), columns, P())
    body = functools.partial(on_device, mesh.shape["gx"], mesh.shape["gy"])
    return jax.shard_map(
        body, mesh=mesh, in_specs=in_specs, out_specs=out_specs, check_vma=False
    )
```

```python
import functools

import jax
import jax.numpy as jnp
from jax import lax
from jax.experimental import pallas as pl
from jax.experimental.pallas import tpu as pltpu
from jax.sharding import PartitionSpec as P

SUB = 512
LANES = 128
STEP = 8
GROUP = 4
ZBLOCK = 32
MESH = pl.DeviceIdType.MESH
VMEM_LIMIT = 48 * 512 * 1024


def flow(p, k, pn, kn):
    return 2.0 * k * kn / (k + kn) * (p - pn)


def split(value):
    high = value.astype(jnp.bfloat16)
    return high, (value - high.astype(jnp.float32)).astype(jnp.bfloat16)


def spread(thick_row, layers):
    rows = lax.broadcasted_iota(jnp.int32, (layers, layers), 0)
    cols = lax.broadcasted_iota(jnp.int32, (layers, layers), 1)
    grid = jnp.broadcast_to(thick_row, (layers, layers))
    column = jnp.sum(jnp.where(rows == cols, grid, 0.0), axis=1, keepdims=True)
    return jnp.broadcast_to(column, (layers, LANES))


def onehot_of(row):
    ids = lax.broadcasted_iota(jnp.int32, (SUB, LANES), 0)
    return jnp.where(ids == row, 1.0, 0.0).astype(jnp.bfloat16)


def nt_dot(a, b):
    return lax.dot_general(
        a, b, (((1,), (1,)), ((), ())), preferred_element_type=jnp.float32
    )


def local_kernel(
    pressure, conduct, sat_new, sat_old, porosity, storage, et_rate, thick, labels, outlet,
    partial, balance, edges, peak,
    p_buf, k_buf, n_buf, o_buf, r_buf, s_buf, e_buf, depth, carry, sums, lhs, hot, total, sems,
):
    layers, cx, cy = pressure.shape
    chunks = cx // STEP
    first = ((pressure, p_buf), (conduct, k_buf))
    rest = ((sat_new, n_buf), (sat_old, o_buf), (porosity, r_buf), (storage, s_buf), (et_rate, e_buf))
    pairs = first + rest

    def fetch(chunk, which):
        for a in which:
            source, target = pairs[a]
            for i in range(STEP):
                x = chunk * STEP + i
                pltpu.make_async_copy(source.at[:, x, :], target.at[x], sems.at[a, chunk]).start()

    def wait(chunk, which):
        for a in which:
            target = pairs[a][1].at[pl.ds(chunk * STEP, STEP)]
            pltpu.make_async_copy(target, target, sems.at[a, chunk]).wait()

    fetch(0, (0, 1))
    for chunk in range(chunks):
        if chunk + 1 < chunks:
            fetch(chunk + 1, (0, 1))
        fetch(chunk, range(2, 7))

    p_buf[cx] = jnp.zeros((layers, cy), jnp.float32)
    k_buf[cx] = jnp.zeros((layers, cy), jnp.float32)
    depth[...] = spread(thick[...], layers)
    carry[...] = jnp.zeros_like(carry)
    total[...] = jnp.zeros_like(total)
    peak[...] = jnp.zeros_like(peak)
    sums[...] = jnp.zeros_like(sums)
    edges[:, 2] = jnp.zeros((2, layers, cy), jnp.float32)
    lane = lax.broadcasted_iota(jnp.int32, (ZBLOCK, cy), 1)
    quarter = 4 * layers
    wait(0, (0, 1))

    def fold(value):
        return jnp.sum(value.reshape(ZBLOCK // 8, 8, cy), axis=0)

    def body(chunk, _):
        @pl.when(chunk + 1 < chunks)
        def _():
            wait(chunk + 1, (0, 1))

        wait(chunk, range(2, 7))
        for sub in range(STEP // GROUP):
            for zi in range(layers // ZBLOCK):
                zs = pl.ds(zi * ZBLOCK, ZBLOCK)
                before = carry[zs]
                d = depth[zs]
                biggest = peak[...]
                for i in range(GROUP):
                    x = chunk * STEP + sub * GROUP + i
                    p = p_buf[x, zs]
                    k = k_buf[x, zs]
                    ahead = flow(p, k, p_buf[x + 1, zs], k_buf[x + 1, zs])
                    side = flow(p, k, pltpu.roll(p, cy - 1, 1), pltpu.roll(k, cy - 1, 1))
                    side = jnp.where(lane < cy - 1, side, 0.0)
                    flux = d * (ahead - before + side - pltpu.roll(side, 1, 1))
                    before = ahead
                    mine = (lane >> 1) == x
                    edges[0, 2, zs] = jnp.where(mine, pltpu.roll(p, 2 * x + 1, 1), edges[0, 2, zs])
                    edges[1, 2, zs] = jnp.where(mine, pltpu.roll(k, 2 * x + 1, 1), edges[1, 2, zs])
                    new = n_buf[x, zs]
                    delta = new - o_buf[x, zs]
                    por = r_buf[x, zs]
                    water = d * new * (por + s_buf[x, zs] * p)
                    change = d * por * delta
                    uptake = d * e_buf[x, zs]
                    biggest = jnp.maximum(
                        biggest, jnp.max(jnp.abs(delta).reshape(ZBLOCK // 8, 8, cy), axis=0)
                    )
                    gate = outlet[pl.ds(x, 1), :].astype(jnp.float32)
                    cols = pl.ds(i * cy, cy)
                    for q, (field, kept) in enumerate(
                        ((water, water), (change, change), (uptake, uptake), (flux, flux * gate))
                    ):
                        sums[q, x] += fold(field)
                        high, low = split(kept)
                        row = q * layers + zi * ZBLOCK
                        lhs[sub, pl.ds(row, ZBLOCK), cols] = high
                        lhs[sub, pl.ds(quarter + row, ZBLOCK), cols] = low
                carry[zs] = before
                peak[...] = biggest
            for i in range(GROUP):
                x = chunk * STEP + sub * GROUP + i
                hot[sub, :, pl.ds(i * cy, cy)] = onehot_of(labels[pl.ds(x, 1), :])
            out = nt_dot(lhs[sub], hot[sub])
            total[...] += out[:quarter] + out[quarter:]
        return 0

    lax.fori_loop(0, chunks, body, 0)
    strips = SUB // LANES
    for q in range(4):
        for c in range(strips):
            block = pl.ds((q * strips + c) * layers, layers)
            partial[block] = total[pl.ds(q * layers, layers), pl.ds(c * LANES, LANES)]
    for q in range(4):
        balance[q] = jnp.sum(sums[q], axis=1)
    for a, buf in enumerate((p_buf, k_buf)):
        edges[a, 0] = buf[0]
        edges[a, 1] = buf[cx - 1]


def stages_of(n1, n2):
    found = []
    if n1 % 2 == 0 and n1 > 2:
        found += [("gx", 1, 2), ("gx", 2, n1 // 2)]
    else:
        found += [("gx", 1, n1)]
    return found + [("gy", 1, n2)]


def shared_kernel(
    n1, n2, slices, scale,
    partial, balance_in, edges, peak_in, thick, labels, outlet,
    totals, balance, peak,
    halo, work, *rest,
):
    stages = stages_of(n1, n2)
    count = len(stages)
    slots = rest[:count]
    blocks = rest[count : 2 * count]
    tiles = rest[2 * count : 3 * count]
    tops, full, halo_send, halo_recv, send, recv, tile_send, tile_recv, back_send, back_recv = rest[3 * count :]
    gx = lax.axis_index("gx")
    gy = lax.axis_index("gy")
    layers = edges.shape[2]
    cx = labels.shape[0]
    cy = labels.shape[1]
    strips = SUB // LANES
    length = 4 * strips * layers // slices
    last = slices - 1
    places = []
    for axis, stride, size in stages:
        me = gx if axis == "gx" else gy
        places.append((axis, me, stride, size, lax.rem(me // stride, size)))
    parts = []
    for _, _, size in stages:
        parts.append((parts[-1] if parts else length) // size)
    pending = []

    def sources(s):
        if s == 0:
            return [partial.at[pl.ds(k * length, length)] for k in range(last)] + [work]
        return [blocks[s - 1].at[k] for k in range(slices)]

    def scatter(s, k):
        axis, me, stride, size, spot = places[s]
        part = parts[s]
        found = []
        for j in range(1, size):
            there = lax.rem(spot + j, size)
            copy = pltpu.make_async_remote_copy(
                src_ref=sources(s)[k].at[pl.ds(pl.multiple_of(there * part, min(part, 8)), part)],
                dst_ref=slots[s].at[k, j - 1],
                send_sem=send.at[s, k, j - 1],
                recv_sem=recv.at[s, k, j - 1],
                device_id={axis: me + (there - spot) * stride},
                device_id_type=MESH,
            )
            copy.start()
            found.append(copy)
        pending.extend(found)
        return found

    def exchange(s):
        axis, me, stride, size, spot = places[s]
        found = []
        for j in range(1, size):
            there = lax.rem(spot + j, size)
            copy = pltpu.make_async_remote_copy(
                src_ref=tops.at[s],
                dst_ref=tiles[s].at[j - 1],
                send_sem=tile_send.at[s, j - 1],
                recv_sem=tile_recv.at[s, j - 1],
                device_id={axis: me + (there - spot) * stride},
                device_id_type=MESH,
            )
            copy.start()
            found.append(copy)
        pending.extend(found)
        return found

    tops[0] = peak_in[...]
    barrier = pltpu.get_barrier_semaphore()
    for axis, me, n in (("gx", gx, n1), ("gy", gy, n2)):
        for j in range(1, n):
            pl.semaphore_signal(barrier, inc=1, device_id={axis: lax.rem(me + j, n)}, device_id_type=MESH)
    pl.semaphore_wait(barrier, n1 + n2 - 2)

    copies = []
    for slot, (axis, me, n, hop, which) in enumerate(
        (("gx", gx, n1, 1, 1), ("gx", gx, n1, n1 - 1, 0), ("gy", gy, n2, 1, 2), ("gy", gy, n2, n2 - 1, 2))
    ):
        copy = pltpu.make_async_remote_copy(
            src_ref=edges.at[:, which],
            dst_ref=halo.at[slot],
            send_sem=halo_send.at[slot],
            recv_sem=halo_recv.at[slot],
            device_id={axis: lax.rem(me + hop, n)},
            device_id_type=MESH,
        )
        copy.start()
        copies.append(copy)
    moving = [scatter(0, k) for k in range(last)]
    top_moving = exchange(0)

    depth = spread(thick[...], layers)
    lane = lax.broadcasted_iota(jnp.int32, (layers, cy), 1)
    place_x = lax.broadcasted_iota(jnp.int32, (cx, cy), 0)
    place_c = lax.broadcasted_iota(jnp.int32, (cx, cy), 1)

    def packed(grid):
        top = jnp.broadcast_to(grid[:, cy - 1 :], (cx, cy))
        low = jnp.broadcast_to(grid[:, :1], (cx, cy))
        spot = jnp.where(place_c == 2 * place_x, top, 0) + jnp.where(place_c == 2 * place_x + 1, low, 0)
        return jnp.sum(spot, axis=0, keepdims=True)

    work[...] = partial[pl.ds(last * length, length)]
    gates = outlet[...].astype(jnp.float32)
    names = labels[...].astype(jnp.float32)
    side_names = packed(names).astype(jnp.int32)
    side_gates = packed(gates)
    hot = jnp.concatenate(
        [onehot_of(labels[pl.ds(0, 1), :]), onehot_of(labels[pl.ds(cx - 1, 1), :]), onehot_of(side_names)], axis=1
    )

    for copy in copies:
        copy.wait()
    inside = (gx > 0, gx < n1 - 1, gy > 0, gy < n2 - 1)
    open_ = [jnp.where(flag, 1.0, 0.0) for flag in inside]
    near_p = [halo[s, 0] for s in range(4)]
    near_k = [halo[s, 1] * open_[s] for s in range(4)]
    low = depth * flow(edges[0, 0], edges[1, 0], near_p[0], near_k[0])
    high = depth * flow(edges[0, 1], edges[1, 1], near_p[1], near_k[1])
    even = (lane & 1) == 0
    side_p = jnp.where(even, pltpu.roll(near_p[3], cy - 1, 1), pltpu.roll(near_p[2], 1, 1))
    side_k = jnp.where(even, pltpu.roll(near_k[3], cy - 1, 1), pltpu.roll(near_k[2], 1, 1))
    own_k = jnp.where(lane < 2 * cx, edges[1, 2], 1.0)
    side = depth * flow(edges[0, 2], own_k, side_p, side_k)
    side = jnp.where(lane < 2 * cx, side, 0.0)
    extra = jnp.concatenate(
        [low * gates[:1], high * gates[cx - 1 :], side * side_gates], axis=1
    )
    up, down = split(extra)
    out = nt_dot(jnp.concatenate([up, down], axis=0), hot)
    out = out[:layers] + out[layers:]
    begin = length - strips * layers
    for c in range(strips):
        work[pl.ds(begin + c * layers, layers)] += out[:, c * LANES : (c + 1) * LANES]
    moving.append(scatter(0, last))

    for s in range(count):
        _, _, _, size, spot = places[s]
        part = parts[s]
        later = []
        for k in range(slices):
            for copy in moving[k]:
                copy.wait_recv()
            mine = pl.multiple_of(spot * part, min(part, 8))
            value = sources(s)[k][pl.ds(mine, part)]
            for j in range(size - 1):
                value = value + slots[s][k, j]
            if s + 1 < count:
                blocks[s][k] = value
                later.append(scatter(s + 1, k))
            else:
                base = 0
                for (_, _, _, _, spot_of), part_of in zip(places, parts):
                    base = base + spot_of * part_of
                full[pl.ds(pl.multiple_of(k * length + base, min(part, 8)), part)] = value * scale
                later.append(gather(s, k, base, places, parts, full, back_send, back_recv, pending))
            if k == 0:
                for copy in top_moving:
                    copy.wait_recv()
                top = tops[s]
                for j in range(size - 1):
                    top = jnp.maximum(top, tiles[s][j])
                tops[s + 1] = top
                top_moving = exchange(s + 1) if s + 1 < count else []
        moving = later

    sum_low = jnp.sum(low, axis=0, keepdims=True)
    sum_high = jnp.sum(high, axis=0, keepdims=True)
    sum_side = jnp.broadcast_to(jnp.sum(side, axis=0, keepdims=True), (cx, cy))
    column_top = jnp.sum(jnp.where(place_c == 2 * place_x, sum_side, 0.0), axis=1, keepdims=True)
    column_low = jnp.sum(jnp.where(place_c == 2 * place_x + 1, sum_side, 0.0), axis=1, keepdims=True)
    more = jnp.where(place_c == cy - 1, column_top, 0.0) + jnp.where(place_c == 0, column_low, 0.0)
    more = more + jnp.where(place_x == 0, sum_low, 0.0) + jnp.where(place_x == cx - 1, sum_high, 0.0)
    balance[pl.ds(0, 3)] = balance_in[pl.ds(0, 3)]
    balance[3] = balance_in[3] + more
    peak[...] = jnp.max(jnp.max(tops[count], axis=0, keepdims=True), axis=1, keepdims=True)

    for s in range(count - 1, -1, -1):
        base = 0
        for (_, _, _, _, spot_of), part_of in zip(places[:s], parts[:s]):
            base = base + spot_of * part_of
        later = []
        for k in range(slices):
            for copy in moving[k]:
                copy.wait_recv()
            if s > 0:
                later.append(gather(s - 1, k, base, places, parts, full, back_send, back_recv, pending))
            else:
                for block in range(k * length // layers, (k + 1) * length // layers):
                    q, c = divmod(block, strips)
                    totals[q, :, pl.ds(c * LANES, LANES)] = full[pl.ds(block * layers, layers)]
        moving = later
    for copy in pending:
        copy.wait_send()


def gather(s, k, base, places, parts, full, back_send, back_recv, pending):
    axis, me, stride, size, spot = places[s]
    part = parts[s]
    length = parts[0] * places[0][3]
    held = full.at[pl.ds(pl.multiple_of(k * length + base, min(part, 8)), part)]
    found = []
    for j in range(1, size):
        there = lax.rem(spot + j, size)
        copy = pltpu.make_async_remote_copy(
            src_ref=held,
            dst_ref=held,
            send_sem=back_send.at[s, k, j - 1],
            recv_sem=back_recv.at[s, k, j - 1],
            device_id={axis: me + (there - spot) * stride},
            device_id_type=MESH,
        )
        copy.start()
        found.append(copy)
    pending.extend(found)
    return found


def on_device(
    n1, n2,
    sat_new, sat_old, porosity, spec_storage, pressure, conduct, et_rate, thickness, labels, outlet
):
    layers, cx, cy = sat_new.shape
    quarter = 4 * layers
    f32 = jnp.float32
    vmem = pl.BlockSpec(memory_space=pltpu.VMEM)
    hbm = pl.BlockSpec(memory_space=pltpu.HBM)
    rows = SUB // LANES * quarter
    thick = thickness.reshape(1, layers)
    slab = pltpu.VMEM((cx, layers, cy), f32)
    slab1 = pltpu.VMEM((cx + 1, layers, cy), f32)
    partial, balance, edges, peak = pl.pallas_call(
        local_kernel,
        out_shape=(
            jax.ShapeDtypeStruct((rows, LANES), f32),
            jax.ShapeDtypeStruct((4, cx, cy), f32),
            jax.ShapeDtypeStruct((2, 3, layers, cy), f32),
            jax.ShapeDtypeStruct((8, cy), f32),
        ),
        in_specs=[hbm] * 7 + [vmem] * 3,
        out_specs=(vmem,) * 4,
        scratch_shapes=[slab1, slab1] + [slab] * 5 + [
            pltpu.VMEM((layers, cy), f32),
            pltpu.VMEM((layers, cy), f32),
            pltpu.VMEM((4, cx, 8, cy), f32),
            pltpu.VMEM((STEP // GROUP, 2 * quarter, GROUP * cy), jnp.bfloat16),
            pltpu.VMEM((STEP // GROUP, SUB, GROUP * cy), jnp.bfloat16),
            pltpu.VMEM((quarter, SUB), f32),
            pltpu.SemaphoreType.DMA((7, cx // STEP)),
        ],
        compiler_params=pltpu.CompilerParams(vmem_limit_bytes=VMEM_LIMIT),
        name="local",
    )(*[pltpu.with_memory_space_constraint(v, pltpu.HBM) for v in (pressure, conduct, sat_new, sat_old, porosity, spec_storage, et_rate)], thick, labels, outlet)

    stages = stages_of(n1, n2)
    count = len(stages)
    widest = max(size for _, _, size in stages) - 1
    slices = max(1, min(4, rows // (8 * n1 * n2)))
    left = rows // slices
    slots, blocks, tiles = [], [], []
    for _, _, size in stages:
        left //= size
        slots.append(pltpu.VMEM((slices, size - 1, left, LANES), f32))
        blocks.append(pltpu.VMEM((slices, left, LANES), f32))
        tiles.append(pltpu.VMEM((size - 1, 8, LANES), f32))
    dma = pltpu.SemaphoreType.DMA
    scale = layers * SUB / (cx * n1 * cy * n2)
    totals, balance, peak = pl.pallas_call(
        functools.partial(shared_kernel, n1, n2, slices, scale),
        out_shape=(
            jax.ShapeDtypeStruct((4, layers, SUB), f32),
            jax.ShapeDtypeStruct((4, cx, cy), f32),
            jax.ShapeDtypeStruct((1, 1), f32),
        ),
        in_specs=[vmem] * 7,
        out_specs=(vmem,) * 3,
        scratch_shapes=[
            pltpu.VMEM((4, 2, layers, cy), f32),
            pltpu.VMEM((rows // slices, LANES), f32),
            *slots, *blocks, *tiles,
            pltpu.VMEM((count + 1, 8, LANES), f32),
            pltpu.VMEM((rows, LANES), f32),
            dma((4,)), dma((4,)),
            dma((count, slices, widest)), dma((count, slices, widest)),
            dma((count, widest)), dma((count, widest)),
            dma((count, slices, widest)), dma((count, slices, widest)),
        ],
        compiler_params=pltpu.CompilerParams(
            collective_id=0, has_side_effects=True, vmem_limit_bytes=16 * 1024 * 1024
        ),
        name="shared",
    )(partial, balance, edges, peak, thick, labels, outlet)
    return totals, balance, peak[0, 0]


def solution(mesh):
    columns = P(None, "gx", "gy")
    in_specs = (columns,) * 7 + (P(), P("gx", "gy"), P("gx", "gy"))
    out_specs = (P(), columns, P())
    body = functools.partial(on_device, mesh.shape["gx"], mesh.shape["gy"])
    return jax.shard_map(
        body, mesh=mesh, in_specs=in_specs, out_specs=out_specs, check_vma=False
    )
```

```python
import functools

import jax
import jax.numpy as jnp
from jax import lax
from jax.experimental import pallas as pl
from jax.experimental.pallas import tpu as pltpu
from jax.sharding import PartitionSpec as P

SUB = 512
LANES = 128
STEP = 8
GROUP = 4
ZBLOCK = 32
MESH = pl.DeviceIdType.MESH
VMEM_LIMIT = 48 * 512 * 1024


def flow(p, k, pn, kn):
    return 2.0 * k * kn / (k + kn) * (p - pn)


def split(value):
    high = value.astype(jnp.bfloat16)
    return high, (value - high.astype(jnp.float32)).astype(jnp.bfloat16)


def spread(thick_row, layers):
    rows = lax.broadcasted_iota(jnp.int32, (layers, layers), 0)
    cols = lax.broadcasted_iota(jnp.int32, (layers, layers), 1)
    grid = jnp.broadcast_to(thick_row, (layers, layers))
    column = jnp.sum(jnp.where(rows == cols, grid, 0.0), axis=1, keepdims=True)
    return jnp.broadcast_to(column, (layers, LANES))


def onehot_of(row):
    ids = lax.broadcasted_iota(jnp.int32, (SUB, LANES), 0)
    return jnp.where(ids == row, 1.0, 0.0).astype(jnp.bfloat16)


def nt_dot(a, b):
    return lax.dot_general(
        a, b, (((1,), (1,)), ((), ())), preferred_element_type=jnp.float32
    )


def local_kernel(
    pressure, conduct, sat_new, sat_old, porosity, storage, et_rate, thick, labels, outlet,
    partial, balance, edges, peak,
    p_buf, k_buf, n_buf, o_buf, r_buf, s_buf, e_buf, depth, carry, sums, lhs, hot, total, sems,
):
    layers, cx, cy = pressure.shape
    chunks = cx // STEP
    first = ((pressure, p_buf), (conduct, k_buf))
    rest = ((sat_new, n_buf), (sat_old, o_buf), (porosity, r_buf), (storage, s_buf), (et_rate, e_buf))
    pairs = first + rest

    def fetch(chunk, which):
        for a in which:
            source, target = pairs[a]
            for i in range(STEP):
                x = chunk * STEP + i
                pltpu.make_async_copy(source.at[:, x, :], target.at[x], sems.at[a, chunk]).start()

    def wait(chunk, which):
        for a in which:
            target = pairs[a][1].at[pl.ds(chunk * STEP, STEP)]
            pltpu.make_async_copy(target, target, sems.at[a, chunk]).wait()

    fetch(0, (0, 1))
    for chunk in range(chunks):
        if chunk + 1 < chunks:
            fetch(chunk + 1, (0, 1))
        fetch(chunk, range(2, 7))

    p_buf[cx] = jnp.zeros((layers, cy), jnp.float32)
    k_buf[cx] = jnp.zeros((layers, cy), jnp.float32)
    depth[...] = spread(thick[...], layers)
    carry[...] = jnp.zeros_like(carry)
    total[...] = jnp.zeros_like(total)
    peak[...] = jnp.zeros_like(peak)
    sums[...] = jnp.zeros_like(sums)
    edges[:, 2] = jnp.zeros((2, layers, cy), jnp.float32)
    lane = lax.broadcasted_iota(jnp.int32, (ZBLOCK, cy), 1)
    quarter = 4 * layers
    wait(0, (0, 1))

    def fold(value):
        return jnp.sum(value.reshape(ZBLOCK // 8, 8, cy), axis=0)

    def body(chunk, _):
        @pl.when(chunk + 1 < chunks)
        def _():
            wait(chunk + 1, (0, 1))

        wait(chunk, range(2, 7))
        for sub in range(STEP // GROUP):
            for zi in range(layers // ZBLOCK):
                zs = pl.ds(zi * ZBLOCK, ZBLOCK)
                before = carry[zs]
                d = depth[zs]
                biggest = peak[...]
                for i in range(GROUP):
                    x = chunk * STEP + sub * GROUP + i
                    p = p_buf[x, zs]
                    k = k_buf[x, zs]
                    ahead = flow(p, k, p_buf[x + 1, zs], k_buf[x + 1, zs])
                    side = flow(p, k, pltpu.roll(p, cy - 1, 1), pltpu.roll(k, cy - 1, 1))
                    side = jnp.where(lane < cy - 1, side, 0.0)
                    flux = d * (ahead - before + side - pltpu.roll(side, 1, 1))
                    before = ahead
                    mine = (lane >> 1) == x
                    edges[0, 2, zs] = jnp.where(mine, pltpu.roll(p, 2 * x + 1, 1), edges[0, 2, zs])
                    edges[1, 2, zs] = jnp.where(mine, pltpu.roll(k, 2 * x + 1, 1), edges[1, 2, zs])
                    new = n_buf[x, zs]
                    delta = new - o_buf[x, zs]
                    por = r_buf[x, zs]
                    water = d * new * (por + s_buf[x, zs] * p)
                    change = d * por * delta
                    uptake = d * e_buf[x, zs]
                    biggest = jnp.maximum(
                        biggest, jnp.max(jnp.abs(delta).reshape(ZBLOCK // 8, 8, cy), axis=0)
                    )
                    gate = outlet[pl.ds(x, 1), :].astype(jnp.float32)
                    cols = pl.ds(i * cy, cy)
                    for q, (field, kept) in enumerate(
                        ((water, water), (change, change), (uptake, uptake), (flux, flux * gate))
                    ):
                        sums[q, x] += fold(field)
                        high, low = split(kept)
                        row = q * layers + zi * ZBLOCK
                        lhs[sub, pl.ds(row, ZBLOCK), cols] = high
                        lhs[sub, pl.ds(quarter + row, ZBLOCK), cols] = low
                carry[zs] = before
                peak[...] = biggest
            for i in range(GROUP):
                x = chunk * STEP + sub * GROUP + i
                hot[sub, :, pl.ds(i * cy, cy)] = onehot_of(labels[pl.ds(x, 1), :])
            out = nt_dot(lhs[sub], hot[sub])
            total[...] += out[:quarter] + out[quarter:]
        return 0

    lax.fori_loop(0, chunks, body, 0)
    strips = SUB // LANES
    for q in range(4):
        for c in range(strips):
            block = pl.ds((q * strips + c) * layers, layers)
            partial[block] = total[pl.ds(q * layers, layers), pl.ds(c * LANES, LANES)]
    for q in range(4):
        balance[q] = jnp.sum(sums[q], axis=1)
    for a, buf in enumerate((p_buf, k_buf)):
        edges[a, 0] = buf[0]
        edges[a, 1] = buf[cx - 1]


def stages_of(n1, n2):
    found = []
    if n1 % 2 == 0 and n1 > 2:
        found += [("gx", 1, 2), ("gx", 2, n1 // 2)]
    else:
        found += [("gx", 1, n1)]
    return found + [("gy", 1, n2)]


def shared_kernel(
    n1, n2, slices, scale,
    partial, balance_in, edges, peak_in, thick, labels, outlet,
    totals, balance, peak,
    halo, work, *rest,
):
    stages = stages_of(n1, n2)
    count = len(stages)
    slots = rest[:count]
    blocks = rest[count : 2 * count]
    tiles = rest[2 * count : 3 * count]
    tops, full, halo_send, halo_recv, send, recv, tile_send, tile_recv, back_send, back_recv = rest[3 * count :]
    gx = lax.axis_index("gx")
    gy = lax.axis_index("gy")
    layers = edges.shape[2]
    cx = labels.shape[0]
    cy = labels.shape[1]
    strips = SUB // LANES
    length = 4 * strips * layers // slices
    last = slices - 1
    places = []
    for axis, stride, size in stages:
        me = gx if axis == "gx" else gy
        places.append((axis, me, stride, size, lax.rem(me // stride, size)))
    parts = []
    for _, _, size in stages:
        parts.append((parts[-1] if parts else length) // size)
    pending = []

    def sources(s):
        if s == 0:
            return [partial.at[pl.ds(k * length, length)] for k in range(last)] + [work]
        return [blocks[s - 1].at[k] for k in range(slices)]

    def scatter(s, k):
        axis, me, stride, size, spot = places[s]
        part = parts[s]
        found = []
        for j in range(1, size):
            there = lax.rem(spot + j, size)
            copy = pltpu.make_async_remote_copy(
                src_ref=sources(s)[k].at[pl.ds(pl.multiple_of(there * part, min(part, 8)), part)],
                dst_ref=slots[s].at[k, j - 1],
                send_sem=send.at[s, k, j - 1],
                recv_sem=recv.at[s, k, j - 1],
                device_id={axis: me + (there - spot) * stride},
                device_id_type=MESH,
            )
            copy.start()
            found.append(copy)
        pending.extend(found)
        return found

    def exchange(s):
        axis, me, stride, size, spot = places[s]
        found = []
        for j in range(1, size):
            there = lax.rem(spot + j, size)
            copy = pltpu.make_async_remote_copy(
                src_ref=tops.at[s],
                dst_ref=tiles[s].at[j - 1],
                send_sem=tile_send.at[s, j - 1],
                recv_sem=tile_recv.at[s, j - 1],
                device_id={axis: me + (there - spot) * stride},
                device_id_type=MESH,
            )
            copy.start()
            found.append(copy)
        pending.extend(found)
        return found

    tops[0] = peak_in[...]
    barrier = pltpu.get_barrier_semaphore()
    for axis, me, n in (("gx", gx, n1), ("gy", gy, n2)):
        for j in range(1, n):
            pl.semaphore_signal(barrier, inc=1, device_id={axis: lax.rem(me + j, n)}, device_id_type=MESH)
    pl.semaphore_wait(barrier, n1 + n2 - 2)

    copies = []
    for slot, (axis, me, n, hop, which) in enumerate(
        (("gx", gx, n1, 1, 1), ("gx", gx, n1, n1 - 1, 0), ("gy", gy, n2, 1, 2), ("gy", gy, n2, n2 - 1, 2))
    ):
        copy = pltpu.make_async_remote_copy(
            src_ref=edges.at[:, which],
            dst_ref=halo.at[slot],
            send_sem=halo_send.at[slot],
            recv_sem=halo_recv.at[slot],
            device_id={axis: lax.rem(me + hop, n)},
            device_id_type=MESH,
        )
        copy.start()
        copies.append(copy)
    moving = [scatter(0, k) for k in range(last)]
    top_moving = exchange(0)

    depth = spread(thick[...], layers)
    lane = lax.broadcasted_iota(jnp.int32, (layers, cy), 1)
    place_x = lax.broadcasted_iota(jnp.int32, (cx, cy), 0)
    place_c = lax.broadcasted_iota(jnp.int32, (cx, cy), 1)

    def packed(grid):
        top = jnp.broadcast_to(grid[:, cy - 1 :], (cx, cy))
        low = jnp.broadcast_to(grid[:, :1], (cx, cy))
        spot = jnp.where(place_c == 2 * place_x, top, 0) + jnp.where(place_c == 2 * place_x + 1, low, 0)
        return jnp.sum(spot, axis=0, keepdims=True)

    work[...] = partial[pl.ds(last * length, length)]
    gates = outlet[...].astype(jnp.float32)
    names = labels[...].astype(jnp.float32)
    side_names = packed(names).astype(jnp.int32)
    side_gates = packed(gates)
    hot = jnp.concatenate(
        [onehot_of(labels[pl.ds(0, 1), :]), onehot_of(labels[pl.ds(cx - 1, 1), :]), onehot_of(side_names)], axis=1
    )

    for copy in copies:
        copy.wait()
    inside = (gx > 0, gx < n1 - 1, gy > 0, gy < n2 - 1)
    open_ = [jnp.where(flag, 1.0, 0.0) for flag in inside]
    near_p = [halo[s, 0] for s in range(4)]
    near_k = [halo[s, 1] * open_[s] for s in range(4)]
    low = depth * flow(edges[0, 0], edges[1, 0], near_p[0], near_k[0])
    high = depth * flow(edges[0, 1], edges[1, 1], near_p[1], near_k[1])
    even = (lane & 1) == 0
    side_p = jnp.where(even, pltpu.roll(near_p[3], cy - 1, 1), pltpu.roll(near_p[2], 1, 1))
    side_k = jnp.where(even, pltpu.roll(near_k[3], cy - 1, 1), pltpu.roll(near_k[2], 1, 1))
    own_k = jnp.where(lane < 2 * cx, edges[1, 2], 1.0)
    side = depth * flow(edges[0, 2], own_k, side_p, side_k)
    side = jnp.where(lane < 2 * cx, side, 0.0)
    extra = jnp.concatenate(
        [low * gates[:1], high * gates[cx - 1 :], side * side_gates], axis=1
    )
    up, down = split(extra)
    out = nt_dot(jnp.concatenate([up, down], axis=0), hot)
    out = out[:layers] + out[layers:]
    begin = length - strips * layers
    for c in range(strips):
        work[pl.ds(begin + c * layers, layers)] += out[:, c * LANES : (c + 1) * LANES]
    moving.append(scatter(0, last))

    for s in range(count):
        _, _, _, size, spot = places[s]
        part = parts[s]
        later = []
        for k in range(slices):
            for copy in moving[k]:
                copy.wait_recv()
            mine = pl.multiple_of(spot * part, min(part, 8))
            value = sources(s)[k][pl.ds(mine, part)]
            for j in range(size - 1):
                value = value + slots[s][k, j]
            if s + 1 < count:
                blocks[s][k] = value
                later.append(scatter(s + 1, k))
            else:
                base = 0
                for (_, _, _, _, spot_of), part_of in zip(places, parts):
                    base = base + spot_of * part_of
                full[pl.ds(pl.multiple_of(k * length + base, min(part, 8)), part)] = value * scale
                later.append(gather(s, k, base, places, parts, full, back_send, back_recv, pending))
            if k == 0:
                for copy in top_moving:
                    copy.wait_recv()
                top = tops[s]
                for j in range(size - 1):
                    top = jnp.maximum(top, tiles[s][j])
                tops[s + 1] = top
                top_moving = exchange(s + 1) if s + 1 < count else []
        moving = later

    sum_low = jnp.sum(low, axis=0, keepdims=True)
    sum_high = jnp.sum(high, axis=0, keepdims=True)
    sum_side = jnp.broadcast_to(jnp.sum(side, axis=0, keepdims=True), (cx, cy))
    column_top = jnp.sum(jnp.where(place_c == 2 * place_x, sum_side, 0.0), axis=1, keepdims=True)
    column_low = jnp.sum(jnp.where(place_c == 2 * place_x + 1, sum_side, 0.0), axis=1, keepdims=True)
    more = jnp.where(place_c == cy - 1, column_top, 0.0) + jnp.where(place_c == 0, column_low, 0.0)
    more = more + jnp.where(place_x == 0, sum_low, 0.0) + jnp.where(place_x == cx - 1, sum_high, 0.0)
    balance[pl.ds(0, 3)] = balance_in[pl.ds(0, 3)]
    balance[3] = balance_in[3] + more
    peak[...] = jnp.max(jnp.max(tops[count], axis=0, keepdims=True), axis=1, keepdims=True)

    for s in range(count - 1, -1, -1):
        base = 0
        for (_, _, _, _, spot_of), part_of in zip(places[:s], parts[:s]):
            base = base + spot_of * part_of
        later = []
        for k in range(slices):
            for copy in moving[k]:
                copy.wait_recv()
            if s > 0:
                later.append(gather(s - 1, k, base, places, parts, full, back_send, back_recv, pending))
            else:
                for block in range(k * length // layers, (k + 1) * length // layers):
                    q, c = divmod(block, strips)
                    totals[q, :, pl.ds(c * LANES, LANES)] = full[pl.ds(block * layers, layers)]
        moving = later
    for copy in pending:
        copy.wait_send()


def gather(s, k, base, places, parts, full, back_send, back_recv, pending):
    axis, me, stride, size, spot = places[s]
    part = parts[s]
    length = parts[0] * places[0][3]
    held = full.at[pl.ds(pl.multiple_of(k * length + base, min(part, 8)), part)]
    found = []
    for j in range(1, size):
        there = lax.rem(spot + j, size)
        copy = pltpu.make_async_remote_copy(
            src_ref=held,
            dst_ref=held,
            send_sem=back_send.at[s, k, j - 1],
            recv_sem=back_recv.at[s, k, j - 1],
            device_id={axis: me + (there - spot) * stride},
            device_id_type=MESH,
        )
        copy.start()
        found.append(copy)
    pending.extend(found)
    return found


def on_device(
    n1, n2,
    sat_new, sat_old, porosity, spec_storage, pressure, conduct, et_rate, thickness, labels, outlet
):
    layers, cx, cy = sat_new.shape
    quarter = 4 * layers
    f32 = jnp.float32
    vmem = pl.BlockSpec(memory_space=pltpu.VMEM)
    hbm = pl.BlockSpec(memory_space=pltpu.HBM)
    rows = SUB // LANES * quarter
    thick = thickness.reshape(1, layers)
    slab = pltpu.VMEM((cx, layers, cy), f32)
    slab1 = pltpu.VMEM((cx + 1, layers, cy), f32)
    partial, balance, edges, peak = pl.pallas_call(
        local_kernel,
        out_shape=(
            jax.ShapeDtypeStruct((rows, LANES), f32),
            jax.ShapeDtypeStruct((4, cx, cy), f32),
            jax.ShapeDtypeStruct((2, 3, layers, cy), f32),
            jax.ShapeDtypeStruct((8, cy), f32),
        ),
        in_specs=[hbm] * 7 + [vmem] * 3,
        out_specs=(vmem,) * 4,
        scratch_shapes=[slab1, slab1] + [slab] * 5 + [
            pltpu.VMEM((layers, cy), f32),
            pltpu.VMEM((layers, cy), f32),
            pltpu.VMEM((4, cx, 8, cy), f32),
            pltpu.VMEM((STEP // GROUP, 2 * quarter, GROUP * cy), jnp.bfloat16),
            pltpu.VMEM((STEP // GROUP, SUB, GROUP * cy), jnp.bfloat16),
            pltpu.VMEM((quarter, SUB), f32),
            pltpu.SemaphoreType.DMA((7, cx // STEP)),
        ],
        compiler_params=pltpu.CompilerParams(vmem_limit_bytes=VMEM_LIMIT),
        name="local",
    )(*[pltpu.with_memory_space_constraint(v, pltpu.HBM) for v in (pressure, conduct, sat_new, sat_old, porosity, spec_storage, et_rate, thick, labels, outlet)])

    stages = stages_of(n1, n2)
    count = len(stages)
    widest = max(size for _, _, size in stages) - 1
    slices = max(1, min(4, rows // (8 * n1 * n2)))
    left = rows // slices
    slots, blocks, tiles = [], [], []
    for _, _, size in stages:
        left //= size
        slots.append(pltpu.VMEM((slices, size - 1, left, LANES), f32))
        blocks.append(pltpu.VMEM((slices, left, LANES), f32))
        tiles.append(pltpu.VMEM((size - 1, 8, LANES), f32))
    dma = pltpu.SemaphoreType.DMA
    scale = layers * SUB / (cx * n1 * cy * n2)
    totals, balance, peak = pl.pallas_call(
        functools.partial(shared_kernel, n1, n2, slices, scale),
        out_shape=(
            jax.ShapeDtypeStruct((4, layers, SUB), f32),
            jax.ShapeDtypeStruct((4, cx, cy), f32),
            jax.ShapeDtypeStruct((1, 1), f32),
        ),
        in_specs=[vmem] * 7,
        out_specs=(vmem,) * 3,
        scratch_shapes=[
            pltpu.VMEM((4, 2, layers, cy), f32),
            pltpu.VMEM((rows // slices, LANES), f32),
            *slots, *blocks, *tiles,
            pltpu.VMEM((count + 1, 8, LANES), f32),
            pltpu.VMEM((rows, LANES), f32),
            dma((4,)), dma((4,)),
            dma((count, slices, widest)), dma((count, slices, widest)),
            dma((count, widest)), dma((count, widest)),
            dma((count, slices, widest)), dma((count, slices, widest)),
        ],
        compiler_params=pltpu.CompilerParams(
            collective_id=0, has_side_effects=True, vmem_limit_bytes=16 * 1024 * 1024
        ),
        name="shared",
    )(partial, balance, edges, peak, thick, labels, outlet)
    return totals, balance, peak[0, 0]


def solution(mesh):
    columns = P(None, "gx", "gy")
    in_specs = (columns,) * 7 + (P(), P("gx", "gy"), P("gx", "gy"))
    out_specs = (P(), columns, P())
    body = functools.partial(on_device, mesh.shape["gx"], mesh.shape["gy"])
    return jax.shard_map(
        body, mesh=mesh, in_specs=in_specs, out_specs=out_specs, check_vma=False
    )
```
